128 devices in a mesh: dp: 8 (over x_hi, y), mp: 16 (over x_lo, z, core).
Axes of the slice: x: 4 (x_hi: 2, x_lo: 2; x = x_hi * 2 + x_lo), y: 4, z: 4, core: 2. Of those that a mesh axis runs over, the one named last changes fastest.
Arguments:
- image: bfloat16 [8, 2048, 1280], P('dp', 'mp'), may hold values from -6 to 6
- ln_gain: float32 [1280], replicated, may hold values from 0.1 to 1.9
- fc1_weight: bfloat16 [1280, 5120], P(None, ('dp', 'mp')), may hold values from -0.15625 to 0.15625
- fc2_weight: bfloat16 [5120, 1280], P(('dp', 'mp')), may hold values from -0.078125 to 0.078125
- projector_weight: bfloat16 [1280, 8192], P(None, 'mp'), may hold values from -0.15625 to 0.15625
- kv_weight: bfloat16 [8192, 8, 2, 128], P('mp'), may hold values from -0.0625 to 0.0625
- text: bfloat16 [8, 128, 8192], P('dp'), may hold values from -480 to 480
- q_weight: bfloat16 [8192, 8192], P(None, 'mp'), may hold values from -0.0625 to 0.0625
- o_weight: bfloat16 [8192, 8192], P('mp'), may hold values from -0.0625 to 0.0625
- tile_count: int32 [8], P('dp'), may hold values from 1 to 4
- text_start: int32 [8], P('dp'), may hold values from 0 to 63
Outputs:
- attended: bfloat16 [8, 128, 8192], P('dp', 'mp')
The draws below stay inside these ranges and needn't reach their ends.
All inputs are finite; a program needn't handle non-finite values.
Results may differ from the reference program's by a relative error of at most 0.035.
Values may be sent and summed in bfloat16 or wider, within the bound.
No kernel may reach another device: no remote copies, remote signals or barrier semaphores. Data moves between devices by JAX's collectives and lax.ppermute only.
A program may use at most 128 MiB of HBM per device.

```python
import jax
import jax.numpy as jnp
from jax import lax

D_VIS = 1280
VIS_FF = 5120
HEADS = 64
KV_HEADS = 8
HEAD_DIM = 128
D = 8192
MAX_TILES = 4
TILE_TOK = 512
TEXT = 128
IMG = 2048
SAMPLES = 8


def draw_text(key, part):
    base = jax.random.normal(key, (SAMPLES, TEXT, D), jnp.float32)
    return jnp.clip(base, -6.0, 6.0).astype(jnp.bfloat16)


def touch_ends(entries, stream_key, low, top_value):
    longest = entries.shape.index(max(entries.shape))
    spots = []
    for shift in (0, 1):
        where = [jax.random.randint(jax.random.fold_in(stream_key, axis), (), 0, length) for axis, length in enumerate(entries.shape)]
        where[longest] = (where[longest] + shift) % entries.shape[longest]
        spots.append(tuple(where))
    return entries.at[spots[0]].set(low).at[spots[1]].set(top_value)


def block_levels(rng, extent, shards, least, largest):
    def one(dim, blocks):
        draws = jax.random.uniform(jax.random.fold_in(jax.random.fold_in(rng, 6), dim), (blocks,), jnp.float32, least / len(shards), largest / len(shards))
        return jnp.repeat(jnp.exp(draws), extent[dim] // blocks).reshape((-1,) + (1,) * (len(extent) - dim - 1))

    level = one(*shards[0])
    for cut in shards[1:]:
        level = level * one(*cut)
    return level


def centred(stream_key, shape, scale, reach, shards=(), held_as=jnp.bfloat16):
    result = jax.random.normal(stream_key, shape, jnp.float32) * scale
    if len(shards) > 0:
        result = block_levels(stream_key, shape, shards, -0.22, 0.18) * result
    return jnp.clip(result, min=-reach, max=reach).astype(held_as)


def setup_inputs(seed: int = 0) -> dict:
    splits = jax.random.split(jax.random.key(seed), 12)
    return {
        "image": centred(splits[0], (SAMPLES, IMG, D_VIS), 1.0, 6.0, ((0, 8), (1, 16))),
        "ln_gain": jnp.clip(1.0 + 0.18 * jax.random.normal(splits[1], (D_VIS,), jnp.float32), 0.1, 1.9),
        "fc1_weight": centred(splits[2], (D_VIS, VIS_FF), D_VIS ** -0.5, 0.15625, ((1, 128),)),
        "fc2_weight": centred(splits[3], (VIS_FF, D_VIS), VIS_FF ** -0.5, 0.078125, ((0, 128),)),
        "projector_weight": centred(splits[4], (D_VIS, D), D_VIS ** -0.5, 0.15625, ((1, 16),)),
        "kv_weight": centred(splits[5], (D, KV_HEADS, 2, HEAD_DIM), D ** -0.5, 0.0625, ((0, 16),)),
        "text": draw_text(jax.random.fold_in(splits[11], 71), 0),
        "q_weight": centred(splits[7], (D, D), D ** -0.5, 0.0625, ((1, 16),)),
        "o_weight": centred(splits[8], (D, D), D ** -0.5, 0.0625, ((0, 16),)),
        "tile_count": touch_ends(jax.random.randint(splits[9], (SAMPLES,), 1, MAX_TILES + 1), jax.random.fold_in(splits[9], 1), 1, MAX_TILES).astype(jnp.int32),
        "text_start": touch_ends(jax.random.randint(splits[10], (SAMPLES,), 0, TEXT // 2), jax.random.fold_in(splits[10], 1), 0, (TEXT // 2) - 1).astype(jnp.int32),
    }


def layer_norm(values, gain):
    center = values - lax.optimization_barrier(jnp.mean(values, axis=-1, keepdims=True))
    spread = lax.optimization_barrier(jnp.mean(center * center, axis=-1, keepdims=True))
    return center * lax.rsqrt(spread + 1e-05) * gain

def reference(image, ln_gain, fc1_weight, fc2_weight, projector_weight, kv_weight, text, q_weight, o_weight, tile_count, text_start):
    group_size = HEADS // KV_HEADS
    scale = 1.0 / HEAD_DIM ** 0.5
    outputs = []
    for sample in range(SAMPLES):
        inputs = image[sample].astype(jnp.float32)
        normed = layer_norm(inputs, ln_gain).astype(jnp.bfloat16)
        hidden = jax.nn.gelu(jnp.dot(normed, fc1_weight, preferred_element_type=jnp.float32), approximate=False).astype(jnp.bfloat16)
        encoded = (inputs + jnp.dot(hidden, fc2_weight, preferred_element_type=jnp.float32)).astype(jnp.bfloat16)
        features = jnp.dot(encoded, projector_weight, preferred_element_type=jnp.float32).astype(jnp.bfloat16)
        projected = jnp.dot(features, kv_weight.reshape(D, KV_HEADS * 2 * HEAD_DIM), preferred_element_type=jnp.float32)
        projected = projected.reshape(IMG, KV_HEADS, 2, HEAD_DIM)
        keys = projected[:, :, 0, :]
        keys = keys * lax.rsqrt(lax.optimization_barrier(jnp.mean(keys * keys, axis=-1, keepdims=True)) + 1e-06)
        keys = keys.astype(jnp.bfloat16)
        values = projected[:, :, 1, :].astype(jnp.bfloat16)
        queries = jnp.dot(text[sample], q_weight, preferred_element_type=jnp.float32).astype(jnp.bfloat16)
        queries = queries.reshape(TEXT, KV_HEADS, group_size, HEAD_DIM).transpose(1, 0, 2, 3)
        tiles = jnp.arange(IMG, dtype=jnp.int32) // TILE_TOK
        valid = tiles < tile_count[sample]

        def one_group(operands):
            group_queries, group_keys, group_values = operands
            scores = jnp.einsum('tgd,kd->gtk', group_queries.astype(jnp.float32), group_keys.astype(jnp.float32)) * scale
            scores = jnp.where(valid[None, None, :], scores, -1e+30)
            top = lax.optimization_barrier(jnp.max(scores, axis=-1, keepdims=True))
            weights = jnp.exp(scores - top)
            probs = (weights / lax.optimization_barrier(jnp.sum(weights, axis=-1, keepdims=True))).astype(jnp.bfloat16)
            return jnp.einsum('gtk,kd->tgd', probs.astype(jnp.float32), group_values.astype(jnp.float32))
        attended_heads = lax.map(one_group, (queries, keys.transpose(1, 0, 2), values.transpose(1, 0, 2)))
        attended_heads = attended_heads.transpose(1, 0, 2, 3).reshape(TEXT, HEADS * HEAD_DIM)
        row_mask = (jnp.arange(TEXT, dtype=jnp.int32) >= text_start[sample]).astype(jnp.float32)
        heads_out = (attended_heads * row_mask[:, None]).astype(jnp.bfloat16)
        outputs.append(jnp.dot(heads_out, o_weight, preferred_element_type=jnp.float32).astype(jnp.bfloat16))
    return jnp.stack(outputs, axis=0)
```

```python
import jax
import jax.numpy as jnp
from jax import lax
from jax.experimental import pallas as pl
from jax.experimental.pallas import tpu as pltpu
from jax.sharding import Mesh, PartitionSpec as P

HEAD_DIM = 128
TILE_TOK = 512
AXES = ("xh", "y", "xl", "z", "c")
SIZES = (2, 4, 2, 4, 2)
BF16 = jnp.bfloat16
F32 = jnp.float32


def flip(block, xh=0, y=0, xl=0, z=0, c=0):
    bits = (xh, y, xl, z, c)
    route = []
    for here in range(128):
        rest, at = here, []
        for size in reversed(SIZES):
            at.append(rest % size)
            rest //= size
        there = 0
        for size, place, bit in zip(SIZES, reversed(at), bits):
            there = there * size + (place ^ bit)
        route.append((here, there))
    return lax.ppermute(block, AXES, route)


def kernel_call(body, outs, args, flops, scalars=None, scratch=()):
    vmem = pl.BlockSpec(memory_space=pltpu.VMEM)
    specs = [vmem] * len(args)
    if scalars is not None:
        specs = [pl.BlockSpec(memory_space=pltpu.SMEM)] + specs
        args = [scalars] + list(args)
    moved = sum(a.size * a.dtype.itemsize for a in list(args) + list(outs))
    return pl.pallas_call(
        body,
        out_shape=list(outs),
        in_specs=specs,
        out_specs=[vmem] * len(outs),
        scratch_shapes=list(scratch),
        compiler_params=pltpu.CompilerParams(vmem_limit_bytes=48 * 2**20),
        cost_estimate=pl.CostEstimate(flops=flops, bytes_accessed=moved, transcendentals=0),
    )(*args)


def out(shape, dtype=BF16):
    return jax.ShapeDtypeStruct(shape, dtype)


def norm_body(image, gain, normed):
    values = image[...].astype(F32)
    center = values - jnp.mean(values, axis=-1, keepdims=True)
    spread = jnp.mean(center * center, axis=-1, keepdims=True)
    normed[...] = (center * lax.rsqrt(spread + 1e-05) * gain[...]).astype(BF16)


def layer_norm(image, gain):
    return kernel_call(norm_body, [out(image.shape)], [image, gain[None]], 10 * image.size)[0]


def stack_body(*refs):
    rows = refs[0].shape[0]
    for k, ref in enumerate(refs[:-1]):
        refs[-1][k * rows : (k + 1) * rows] = ref[...]


def stack(blocks):
    rows, columns = blocks[0].shape
    shape = (rows * len(blocks), columns)
    return kernel_call(stack_body, [out(shape)], blocks, rows * columns)[0]


ROWS = 256


def mlp_rows(rows, up, down, result):
    def step(i, _):
        at = pl.ds(pl.multiple_of(i * ROWS, ROWS), ROWS)
        hidden = dot_nt(rows[at, :], up[...])
        hidden = hidden * (0.5 + 0.5 * lax.erf(hidden * 0.5**0.5))
        result[at, :] = dot(hidden.astype(BF16), down[...]).astype(result.dtype)
        return 0

    lax.fori_loop(0, rows.shape[0] // ROWS, step, 0)


def mlp_first_body(*refs):
    rows, ups, downs = refs[0], refs[1:5], refs[5:9]
    result, up, down = refs[9:]
    for i in range(4):
        up[160 * i : 160 * i + 160] = ups[i][...]
        for j in range(4):
            at = 160 * j + 40 * i
            down[at : at + 40] = downs[i][40 * j : 40 * j + 40]
    mlp_rows(rows, up, down, result)


def mlp_body(rows, up, down, result):
    mlp_rows(rows, up, down, result)


def kv_body(at, encoded, partner, *refs):
    folds, result, rows = refs[:4], refs[4], refs[5]
    c, xl, xh, y = at[0], at[1], at[2], at[3]
    size = encoded.shape[0]
    half = encoded.shape[1] // 2
    rows[pl.ds(pl.multiple_of(c * size, size), size), :] = encoded[...]
    rows[pl.ds(pl.multiple_of((1 - c) * size, size), size), :] = partner[...]
    for k in range(4):
        for h in range(2):
            low = pl.multiple_of(2 * half * h + xl * half, half)
            high = pl.multiple_of(2 * half * h + (1 - xl) * half, half)
            block = dot(rows[:, :half], folds[k][pl.ds(low, half), :])
            block += dot(rows[:, half:], folds[k][pl.ds(high, half), :])
            scale = lax.rsqrt(jnp.mean(block * block, axis=-1, keepdims=True) + 1e-06)
            block = block * jnp.where(c == 0, scale, 1.0)
            result[(xh ^ h) * 4 + (y ^ k)] = block.astype(BF16)


X_BITS = ((0, 0), (0, 1), (1, 0), (1, 1))


def over_x(block):
    return [block] + [flip(block, xh=h, xl=l) for h, l in X_BITS[1:]]


def over_y(block):
    return [block] + [flip(block, y=k) for k in (1, 2, 3)]


def dot(a, b):
    return jnp.dot(a, b, preferred_element_type=F32)


def dot_nt(a, b):
    return lax.dot_general(a, b, (((1,), (1,)), ((), ())), preferred_element_type=F32)


def local(
    image,
    ln_gain,
    fc1_weight,
    fc2_weight,
    projector_weight,
    kv_weight,
    text,
    q_weight,
    o_weight,
    tile_count,
    text_start,
):
    xh, y, xl, z, c = (lax.axis_index(a) for a in AXES)

    ups = over_x(fc1_weight.T)
    downs = over_y(fc2_weight)
    normed = layer_norm(image[0], ln_gain)
    ups = over_y(stack(ups))
    downs = over_x(stack(downs))
    rows = stack([normed] + [flip(normed, z=k) for k in (1, 2, 3)])
    rows_other = flip(rows, c=1)

    head = xh * 4 + y
    part = lax.dynamic_index_in_dim(kv_weight, head, 1, keepdims=False)
    mine = lax.dynamic_index_in_dim(part, c, 1, keepdims=False)
    other = lax.dynamic_index_in_dim(part, 1 - c, 1, keepdims=False)
    fold_other = dot(projector_weight, other).astype(BF16)
    fold = dot(projector_weight, mine) + flip(fold_other, c=1).astype(F32)
    half = fold.shape[0] // 2
    fold_send = lax.dynamic_slice_in_dim(fold, (1 - xl) * half, half, 0).astype(BF16)
    fold = lax.dynamic_slice_in_dim(fold, xl * half, half, 0) + flip(fold_send, xl=1).astype(F32)
    fold_send = fold.astype(BF16)
    fold = fold + sum(flip(fold_send, z=k).astype(F32) for k in (1, 2, 3))
    fold_x = stack(over_x(fold.astype(BF16)))
    fold_y = over_y(fold_x)

    text_rows = text.shape[1]
    local_heads = q_weight.shape[1] // HEAD_DIM
    queries = dot(text[0], q_weight).astype(BF16).reshape(8, 2, 8, -1)
    queries = jnp.where(c == 0, queries, queries[:, ::-1]).transpose(1, 0, 2, 3)
    queries = queries.reshape(text_rows, local_heads, HEAD_DIM)
    queries, rows_other = lax.optimization_barrier((queries, rows_other))

    full, units = rows.shape, 4 * ups[0].shape[0]
    flops = 4 * full[0] * full[1] * units
    weights = out((units, full[1]))
    branch_other, up, down = kernel_call(
        mlp_first_body, [out(full), weights, weights], [rows_other, *ups, *downs], flops
    )
    branch = kernel_call(mlp_body, [out(full, F32)], [rows, up, down], flops)[0]
    branch = branch + flip(branch_other, c=1).astype(F32)
    sent = branch[128:].astype(BF16)
    encoded = image[0].astype(F32) + branch[:128]
    for k in (1, 2, 3):
        encoded = encoded + flip(sent[128 * (k - 1) : 128 * k], z=k).astype(F32)
    encoded = encoded.astype(BF16)

    partner = flip(encoded, c=1)
    size = 2 * encoded.shape[0]
    projected = kernel_call(
        kv_body,
        [out((8, size, HEAD_DIM))],
        [encoded, partner, *fold_y],
        16 * size * full[1] * HEAD_DIM,
        jnp.stack([c, xl, xh, y]),
        [pltpu.VMEM((size, full[1]), BF16)],
    )[0]
    held = lax.all_to_all(projected, ("xl", "z"), 0, 0, tiled=True).reshape(-1, HEAD_DIM)
    valid = jnp.arange(held.shape[0], dtype=jnp.int32) // TILE_TOK < tile_count[0]
    held_other = flip(held, c=1)
    keys = jnp.where(c == 0, held, held_other)
    values = jnp.where(c == 0, held_other, held)

    scores = jnp.einsum("thd,kd->htk", queries, keys, preferred_element_type=F32)
    scores = jnp.where(valid[None, None, :], scores * (1.0 / HEAD_DIM**0.5), -1e30)
    top = jnp.max(scores, axis=-1, keepdims=True)
    weights = jnp.exp(scores - top)
    probs = (weights / jnp.sum(weights, axis=-1, keepdims=True)).astype(BF16)
    attended = jnp.einsum("htk,kd->thd", probs, values, preferred_element_type=F32)
    attended = attended.reshape(text_rows, local_heads * HEAD_DIM)
    row = jnp.arange(text_rows, dtype=jnp.int32)
    position = row % 64 // 8 * 16 + (row // 64 ^ c) * 8 + row % 8
    row_mask = (position >= text_start[0]).astype(F32)
    heads_out = (attended * row_mask[:, None]).astype(BF16)

    terms = dot(heads_out, o_weight)
    terms = terms[:64] + flip(terms[64:].astype(BF16), c=1).astype(F32)
    parts = lax.all_to_all(terms.astype(BF16), ("xl", "z"), 0, 0, tiled=True)
    total = jnp.sum(parts.reshape(8, 8, -1).astype(F32), axis=0)
    return total.astype(BF16)[None]


def solution(mesh):
    grid = Mesh(mesh.devices.reshape(SIZES), AXES)
    dp, mp, every = ("xh", "y"), ("xl", "z", "c"), AXES
    return jax.shard_map(
        local,
        mesh=grid,
        in_specs=(
            P(dp, mp, None),
            P(),
            P(None, every),
            P(every, None),
            P(None, mp),
            P(mp, None, None, None),
            P(dp, None, None),
            P(None, mp),
            P(mp, None),
            P(dp),
            P(dp),
        ),
        out_specs=P(dp, mp, None),
        check_vma=False,
    )
```
